32 devices in a mesh: aa: 8 (over y, x, core), ba: 4 (over z).
Axes of the slice: x: 2, y: 2, z: 4, core: 2. Of those that a mesh axis runs over, the one named last changes fastest.
Arguments:
- query: bfloat16 [3072, 4096], P('aa', 'ba'), may hold values from -28 to 28
- keys: bfloat16 [3072, 2048], P('aa', 'ba'), may hold values from -6 to 6
- values: bfloat16 [3072, 2048], P('aa', 'ba'), may hold values from -6 to 6
- grad_out: bfloat16 [3072, 5376], P('aa', 'ba'), may hold values from -6 to 6
- segment_ids: int32 [3072], P('aa'), may hold values from 0 to 5, never falling along the last dimension, each value on 1 to 1920 neighbouring positions
- w_query: bfloat16 [5376, 4096], P(None, 'ba'), may hold values from -0.125 to 0.125
- w_key: bfloat16 [5376, 2048], P(None, 'ba'), may hold values from -0.1875 to 0.1875
- w_value: bfloat16 [5376, 2048], P(None, 'ba'), may hold values from -0.1875 to 0.1875
- w_out: bfloat16 [4096, 5376], P('ba'), may hold values from -0.078125 to 0.078125
Outputs:
- grad_input: bfloat16 [3072, 5376], P('aa', 'ba')
The draws below stay inside these ranges and needn't reach their ends.
Inputs may be any that keep to these rules, and one draw needn't show every extreme that they name: `segment_ids`: never falls along the sequence; each document has at most 1920 positions.
All inputs are finite; a program needn't handle non-finite values.
Results may differ from the reference program's by a relative error of at most 0.019.
Values may be sent and summed in bfloat16 or wider, within the bound.
A program may use at most 128 MiB of HBM per device.

```python
import math
import jax
import jax.numpy as jnp
import numpy as np
from jax import lax

D = 5376
HQ = 32
KVH = 16
HD = 128
DOCS = 6
TOKENS = 3072
DOC_MOST = 1920


def query_key_pair(key):
    base = jax.random.fold_in(key, 4111)
    key_q, key_k = jax.random.split(base, 2)
    query = jax.random.truncated_normal(key_q, -6.0, 6.0, (TOKENS, KVH, 2, HD), jnp.float32)
    keys = jax.random.truncated_normal(key_k, -6.0, 6.0, (TOKENS, KVH, HD), jnp.float32)
    return (query.reshape(TOKENS, HQ * HD), keys.reshape(TOKENS, KVH * HD))


def draw_query(key, part):
    return query_key_pair(key)[0].astype(jnp.bfloat16)


def draw_keys(key, part):
    return query_key_pair(key)[1].astype(jnp.bfloat16)


def spiked(array, key, source, target, parts, factor):
    def block_of(dim):
        return (jnp.arange(array.shape[dim]) // (array.shape[dim] // parts)).reshape((-1,) + (1,) * (array.ndim - 1 - dim))

    first = jax.random.permutation(key, parts)[block_of(target)]
    far = (block_of(target) + parts // 2) % parts
    return jnp.where((block_of(source) == first) | (block_of(source) == far), factor * array, array)


def shard_levels(stream_key, dims, cuts, smallest, largest):
    def one(axis_at, blocks):
        heights = jax.random.uniform(jax.random.fold_in(jax.random.fold_in(stream_key, 6), axis_at), (blocks,), jnp.float32, smallest / len(cuts), largest / len(cuts))
        return jnp.repeat(jnp.exp(heights), dims[axis_at] // blocks).reshape((-1,) + (1,) * (len(dims) - axis_at - 1))

    gain = one(*cuts[0])
    for cut in cuts[1:]:
        gain = gain * one(*cut)
    return gain


def split_up(number_of, total, limit, lean):
    weights = [(1 << 20) // math.isqrt(rank ** lean) + 1 for rank in range(2, number_of + 1)]
    spare, counts = total - limit - (number_of - 1), [1] * (number_of - 1)
    while spare > 0:
        movable = [i for i in range(number_of - 1) if counts[i] < limit]
        pool, remaining = sum([weights[i] for i in movable]), spare
        for i in movable:
            extra = min(limit - counts[i], max(1, remaining * weights[i] // pool), spare)
            counts[i] = counts[i] + extra
            spare = spare - extra
    return np.array([limit] + counts)


def uneven_parts(own_key, amount, total, most, lean):
    if amount == 2:
        one = jax.random.randint(own_key, (), max(1, total - most), min(most, total - 1) + 1)
        return jnp.stack([one, total - one])
    tallies = jnp.asarray(split_up(amount, total, most, lean), jnp.int32)
    twos = (amount - 1) // 2
    giver, receiver = tallies[1:1 + 2 * twos:2], tallies[2:2 + 2 * twos:2]
    room = jnp.minimum(giver - 1, most - receiver)
    moved = jax.random.randint(jax.random.fold_in(own_key, 1), (twos,), 0, 1 << 20) % (room + 1)
    tallies = tallies.at[1:1 + 2 * twos:2].set(giver - moved).at[2:2 + 2 * twos:2].set(receiver + moved)
    return tallies[jax.random.permutation(jax.random.fold_in(own_key, 2), amount)]


def noise(own_key, extent, width, limit, cuts=(), held_as=jnp.bfloat16):
    drawn = jax.random.normal(own_key, extent, jnp.float32) * width
    if len(cuts) > 0:
        drawn = shard_levels(own_key, extent, cuts, -0.22, 0.18) * drawn
    return jnp.clip(drawn, min=-limit, max=limit).astype(held_as)


def noise_with(key, shape, width, reach, cuts, heavy, kind=jnp.bfloat16):
    entries = width * jax.random.normal(key, shape, jnp.float32)
    if cuts:
        entries = entries * shard_levels(key, shape, cuts, -0.22, 0.18)
    return jnp.clip(spiked(entries, jax.random.fold_in(key, 3), *heavy), -reach, reach).astype(kind)


def setup_inputs(seed: int = 0) -> dict:
    key_of = jax.random.split(jax.random.key(seed), 10)
    return {
        "query": draw_query(jax.random.fold_in(key_of[9], 71), 0),
        "keys": draw_keys(jax.random.fold_in(key_of[9], 71), 0),
        "values": noise(key_of[2], (TOKENS, KVH * HD), 1.0, 6.0, ((0, 8), (1, 4))),
        "grad_out": noise(key_of[3], (TOKENS, D), 1.0, 6.0, ((0, 8), (1, 4))),
        "segment_ids": jnp.searchsorted(jnp.cumsum(uneven_parts(key_of[4], DOCS, TOKENS, DOC_MOST, 1)), jnp.arange(TOKENS), side="right").astype(jnp.int32),
        "w_query": noise_with(key_of[5], (D, HQ * HD), (HQ * HD) ** -0.5, 0.125, ((1, 4),), (1, 0, 4, 2.0)),
        "w_key": noise_with(key_of[6], (D, KVH * HD), (KVH * HD) ** -0.5, 0.1875, ((1, 4),), (1, 0, 4, 2.0)),
        "w_value": noise_with(key_of[7], (D, KVH * HD), (KVH * HD) ** -0.5, 0.1875, ((1, 4),), (1, 0, 4, 2.0)),
        "w_out": noise(key_of[8], (HQ * HD, D), D ** -0.5, 0.078125, ((0, 4),)),
    }


NEG_FILL = -1e30


def back_project(grad, weight):
    return lax.dot_general(grad, weight, (((1,), (1,)), ((), ())), preferred_element_type=jnp.float32)


def reference(query, keys, values, grad_out, segment_ids, w_query, w_key, w_value, w_out):
    scaling = (D / HQ) ** -0.5
    dout = back_project(grad_out, w_out).astype(jnp.bfloat16)
    position = jnp.arange(TOKENS, dtype=jnp.int32)
    allowed = (position[None, :] <= position[:, None]) & (segment_ids[None, :] == segment_ids[:, None])
    query_grp = query.reshape(TOKENS, KVH, 2, HD).transpose(1, 0, 2, 3)
    dout_grp = dout.reshape(TOKENS, KVH, 2, HD).transpose(1, 0, 2, 3)
    keys_grp = keys.reshape(TOKENS, KVH, HD).transpose(1, 0, 2)
    values_grp = values.reshape(TOKENS, KVH, HD).transpose(1, 0, 2)
    highest = lax.Precision.HIGHEST

    def one_group(items):
        query_four, dout_four, key_three, value_three = items
        query_f = query_four.astype(jnp.float32)
        dout_f = dout_four.astype(jnp.float32)
        key_f = key_three.astype(jnp.float32)
        value_f = value_three.astype(jnp.float32)
        scores = jnp.einsum("igd,jd->gij", query_f, key_f, precision=highest) * scaling
        masked = jnp.where(allowed, scores, NEG_FILL)
        top_val = jnp.max(masked, axis=-1)
        expo = jnp.where(allowed, jnp.exp(scores - top_val[..., None]), 0.0)
        lse = top_val + jnp.log(jnp.sum(expo, axis=-1))
        probs = jnp.where(allowed, jnp.exp(scores - lse[..., None]), 0.0)
        dprobs = jnp.einsum("igd,jd->gij", dout_f, value_f, precision=highest)
        delta = jnp.sum(probs * dprobs, axis=-1)
        dscores = probs * (dprobs - delta[..., None])
        probs_low = lax.optimization_barrier(probs.astype(jnp.bfloat16)).astype(jnp.float32)
        dscores_low = lax.optimization_barrier(dscores.astype(jnp.bfloat16)).astype(jnp.float32)
        grad_v = jnp.einsum("gij,igd->jd", probs_low, dout_f, precision=highest)
        grad_k = jnp.einsum("gij,igd->jd", dscores_low, query_f, precision=highest) * scaling
        grad_q = jnp.einsum("gij,jd->igd", dscores_low, key_f, precision=highest) * scaling
        return grad_q, grad_k, grad_v

    grad_q, grad_k, grad_v = lax.map(one_group, (query_grp, dout_grp, keys_grp, values_grp))
    grad_q = grad_q.transpose(1, 0, 2, 3).reshape(TOKENS, HQ * HD).astype(jnp.bfloat16)
    grad_k = grad_k.transpose(1, 0, 2).reshape(TOKENS, KVH * HD).astype(jnp.bfloat16)
    grad_v = grad_v.transpose(1, 0, 2).reshape(TOKENS, KVH * HD).astype(jnp.bfloat16)
    total = back_project(grad_q, w_query) + back_project(grad_k, w_key) + back_project(grad_v, w_value)
    return total.astype(jnp.bfloat16)
```

```python
import functools

import jax
import jax.numpy as jnp
from jax import lax
from jax.experimental import pallas as pl
from jax.experimental.pallas import tpu as pltpu
from jax.sharding import PartitionSpec as P

D = 5376
HQ = 32
HD = 128
DOCS = 6


NEG_FILL = -1e30


def from_behind(value, axis, steps):
    count = lax.axis_size(axis)
    pairs = [(source, (source + steps) % count) for source in range(count)]
    return lax.ppermute(value, axis, pairs)


def block_scores(query, dout, keys, values, query_pos, query_seg, key_pos, key_seg, scaling):
    row_count = query.shape[0]
    col_count = keys.shape[0]
    groups = keys.shape[1] // HD
    query_four = query.reshape(row_count, groups, 2, HD)
    dout_four = dout.reshape(row_count, groups, 2, HD)
    key_three = keys.reshape(col_count, groups, HD)
    value_three = values.reshape(col_count, groups, HD)
    scores = (
        jnp.einsum("iagd,jad->agij", query_four, key_three, preferred_element_type=jnp.float32)
        * scaling
    )
    dprobs = jnp.einsum(
        "iagd,jad->agij", dout_four, value_three, preferred_element_type=jnp.float32
    )
    allowed = (key_pos[None, :] <= query_pos[:, None]) & (key_seg[None, :] == query_seg[:, None])
    return (scores, dprobs, allowed, query_four, dout_four, key_three)


def forward_stats(
    query, dout, keys, values, query_pos, query_seg, key_pos, key_seg, scaling, state
):
    run_max, run_sum, run_dot = state
    scores, dprobs, allowed, unused_q, unused_d, unused_k = block_scores(
        query, dout, keys, values, query_pos, query_seg, key_pos, key_seg, scaling
    )
    masked = jnp.where(allowed, scores, NEG_FILL)
    new_max = jnp.maximum(run_max, jnp.max(masked, axis=-1))
    expo = jnp.where(allowed, jnp.exp(scores - new_max[..., None]), 0.0)
    return (new_max, jnp.sum(expo, axis=-1), jnp.sum(expo * dprobs, axis=-1))


def block_grads(
    query, dout, row_lse, row_delta, keys, values, query_pos, query_seg, key_pos, key_seg, scaling
):
    scores, dprobs, allowed, query_four, dout_four, key_three = block_scores(
        query, dout, keys, values, query_pos, query_seg, key_pos, key_seg, scaling
    )
    softmax_w = jnp.where(allowed, jnp.exp(scores - row_lse[..., None]), 0.0)
    dscores = softmax_w * (dprobs - row_delta[..., None])
    softmax_low = softmax_w.astype(jnp.bfloat16)
    dscores_low = dscores.astype(jnp.bfloat16)
    grad_v = jnp.einsum(
        "agij,iagd->jad", softmax_low, dout_four, preferred_element_type=jnp.float32
    )
    grad_k = (
        jnp.einsum("agij,iagd->jad", dscores_low, query_four, preferred_element_type=jnp.float32)
        * scaling
    )
    grad_q = (
        jnp.einsum("agij,jad->iagd", dscores_low, key_three, preferred_element_type=jnp.float32)
        * scaling
    )
    return (
        grad_q.reshape(query.shape[0], -1),
        grad_k.reshape(keys.shape[0], -1),
        grad_v.reshape(keys.shape[0], -1),
    )


def project_back(grad, weight):
    return lax.dot_general(
        grad, weight, (((1,), (1,)), ((), ())), preferred_element_type=jnp.float32
    )


def local_ring(query, keys, values, grad_out, segment_ids, w_query, w_key, w_value, w_out):
    seq_devices = lax.axis_size("aa")
    own_index = lax.axis_index("aa")
    tok_count = query.shape[0]
    scaling = (D / HQ) ** (-0.5)
    groups = keys.shape[1] // HD
    all_seg = lax.all_gather(segment_ids, "aa", axis=0, tiled=True)
    dout = project_back(lax.all_gather(grad_out, "ba", axis=1, tiled=True), w_out).astype(
        jnp.bfloat16
    )
    offsets = lax.iota(jnp.int32, tok_count)
    own_pos = own_index * tok_count + offsets
    own_seg = lax.dynamic_slice_in_dim(all_seg, own_index * tok_count, tok_count)
    stat_shape = (groups, 2, tok_count)
    stats_start = (
        jnp.full(stat_shape, NEG_FILL, jnp.float32),
        jnp.zeros(stat_shape, jnp.float32),
        jnp.zeros(stat_shape, jnp.float32),
    )
    piece = (
        lax.all_gather(keys, "aa", axis=0, tiled=True),
        lax.all_gather(values, "aa", axis=0, tiled=True),
    )
    width = piece[0].shape[0]
    key_pos = lax.iota(jnp.int32, width)
    key_seg = all_seg
    run_max, run_sum, run_dot = forward_stats(
        query, dout, piece[0], piece[1], own_pos, own_seg, key_pos, key_seg, scaling, stats_start
    )
    row_lse = run_max + jnp.log(run_sum)
    row_delta = run_dot / run_sum
    zero_q = jnp.zeros(query.shape, jnp.float32)
    zero_k = jnp.zeros(keys.shape, jnp.float32)

    def step_keys(step_index, state):
        (keys_now, values_now), (dk_now, dv_now), grad_q = state
        anchor = (own_index - step_index) % seq_devices
        key_pos = anchor * tok_count + offsets
        key_seg = lax.dynamic_slice_in_dim(all_seg, anchor * tok_count, tok_count)
        add_q, add_k, add_v = block_grads(
            query,
            dout,
            row_lse,
            row_delta,
            keys_now,
            values_now,
            own_pos,
            own_seg,
            key_pos,
            key_seg,
            scaling,
        )
        bundle_next = from_behind((keys_now, values_now), "aa", 1)
        sums_next = (
            from_behind((dk_now + add_k).astype(jnp.bfloat16), "aa", 1).astype(jnp.float32),
            from_behind((dv_now + add_v).astype(jnp.bfloat16), "aa", 1).astype(jnp.float32),
        )
        return (bundle_next, sums_next, grad_q + add_q)

    initial = ((keys, values), (zero_k, zero_k), zero_q)
    final = lax.fori_loop(0, seq_devices, step_keys, initial)
    grad_q = final[2]
    grad_k = final[1][0]
    grad_v = final[1][1]
    partial_value = (
        project_back(grad_q.astype(jnp.bfloat16), w_query)
        + project_back(grad_k.astype(jnp.bfloat16), w_key)
        + project_back(grad_v.astype(jnp.bfloat16), w_value)
    )
    return lax.psum_scatter(
        partial_value.astype(jnp.bfloat16), "ba", scatter_dimension=1, tiled=True
    )


def fold_rows(value, op):
    return op(value.reshape(-1, 8, value.shape[1]), axis=0)


def attention_kernel(block, scaling, low_ref, start_ref, qkv_ref, dout_ref, out_ref, s_ref, dp_ref, dk_ref, dv_ref):
    total = qkv_ref.shape[0]
    contract_last = (((1,), (1,)), ((), ()))
    dk_ref[...] = jnp.zeros_like(dk_ref)
    dv_ref[...] = jnp.zeros_like(dv_ref)
    lane = lax.broadcasted_iota(jnp.int32, (block, block), 1)
    sub = lax.broadcasted_iota(jnp.int32, (block, block), 0)

    def query_block(qb, carry):
        rows = pl.ds(pl.multiple_of(qb * block, block), block)
        query = qkv_ref[rows, 0:HD]
        dout = dout_ref[rows, :]
        low = low_ref[qb]
        starts = start_ref[pl.ds(qb, 1), :]

        def scores_at(kb, top):
            cols = pl.ds(pl.multiple_of(kb * block, block), block)
            s = lax.dot_general(qkv_ref[cols, HD : 2 * HD], query, contract_last, preferred_element_type=jnp.float32)
            dp = lax.dot_general(qkv_ref[cols, 2 * HD : 3 * HD], dout, contract_last, preferred_element_type=jnp.float32)
            key_pos = kb * block + sub
            allowed = (key_pos <= qb * block + lane) & (key_pos >= starts)
            s = jnp.where(allowed, s * scaling, NEG_FILL)
            s_ref[cols, :] = s
            dp_ref[cols, :] = dp
            return jnp.maximum(top, fold_rows(s, jnp.max))

        top = lax.fori_loop(low, qb + 1, scores_at, jnp.full((8, block), NEG_FILL, jnp.float32))
        top = jnp.max(top, axis=0, keepdims=True)

        def sums_at(kb, state):
            run_sum, run_dot = state
            cols = pl.ds(pl.multiple_of(kb * block, block), block)
            expo = jnp.exp(s_ref[cols, :] - top)
            s_ref[cols, :] = expo
            return (run_sum + fold_rows(expo, jnp.sum), run_dot + fold_rows(expo * dp_ref[cols, :], jnp.sum))

        zero = jnp.zeros((8, block), jnp.float32)
        run_sum, run_dot = lax.fori_loop(low, qb + 1, sums_at, (zero, zero))
        inverse = 1.0 / jnp.sum(run_sum, axis=0, keepdims=True)
        delta = jnp.sum(run_dot, axis=0, keepdims=True) * inverse

        def grads_at(kb, grad_q):
            cols = pl.ds(pl.multiple_of(kb * block, block), block)
            probs = s_ref[cols, :] * inverse
            dscores = (probs * (dp_ref[cols, :] - delta)).astype(jnp.bfloat16)
            dv_ref[cols, :] += jnp.dot(probs.astype(jnp.bfloat16), dout, preferred_element_type=jnp.float32)
            dk_ref[cols, :] += jnp.dot(dscores, query, preferred_element_type=jnp.float32)
            return grad_q + lax.dot_general(
                dscores, qkv_ref[cols, HD : 2 * HD], (((0,), (0,)), ((), ())), preferred_element_type=jnp.float32
            )

        grad_q = lax.fori_loop(low, qb + 1, grads_at, jnp.zeros((block, HD), jnp.float32))
        out_ref[rows, 0:HD] = (grad_q * scaling).astype(jnp.bfloat16)
        return carry

    lax.fori_loop(0, total // block, query_block, 0)
    out_ref[:, HD : 2 * HD] = (dk_ref[...] * scaling).astype(jnp.bfloat16)
    out_ref[:, 2 * HD : 3 * HD] = dv_ref[...].astype(jnp.bfloat16)


def one_head(qkv, dout, all_seg, scaling):
    total = qkv.shape[0]
    block = 256 if total % 256 == 0 else 128
    firsts = jnp.sum(all_seg[None, :] < lax.iota(jnp.int32, DOCS)[:, None], axis=1, dtype=jnp.int32)
    chosen = all_seg[None, :] == lax.iota(jnp.int32, DOCS)[:, None]
    starts = jnp.sum(jnp.where(chosen, firsts[:, None], 0), axis=0, dtype=jnp.int32).reshape(-1, block)
    low = starts[:, 0] // block
    whole = pl.BlockSpec(memory_space=pltpu.VMEM)
    return pl.pallas_call(
        functools.partial(attention_kernel, block, scaling),
        out_shape=jax.ShapeDtypeStruct((total, 3 * HD), jnp.bfloat16),
        in_specs=[pl.BlockSpec(memory_space=pltpu.SMEM), whole, whole, whole],
        out_specs=whole,
        scratch_shapes=[
            pltpu.VMEM((total, block), jnp.float32),
            pltpu.VMEM((total, block), jnp.float32),
            pltpu.VMEM((total, HD), jnp.float32),
            pltpu.VMEM((total, HD), jnp.float32),
        ],
        compiler_params=pltpu.CompilerParams(vmem_limit_bytes=32 * 1024 * 1024),
        name="attention",
    )(low, starts, qkv, dout)


def local(query, keys, values, grad_out, segment_ids, w_query, w_key, w_value, w_out):
    seq_devices = lax.axis_size("aa")
    tok_count = query.shape[0]
    heads = query.shape[1] // HD
    groups = keys.shape[1] // HD
    if heads != seq_devices:
        return local_ring(query, keys, values, grad_out, segment_ids, w_query, w_key, w_value, w_out)
    scaling = (D / HQ) ** (-0.5)
    all_seg = lax.all_gather(segment_ids, "aa", axis=0, tiled=True)

    def by_head(value):
        return value.reshape(tok_count, -1, HD).transpose(1, 0, 2)

    send = jnp.concatenate(
        [by_head(query), jnp.repeat(by_head(keys), 2, axis=0), jnp.repeat(by_head(values), 2, axis=0)], axis=2
    )
    qkv = lax.all_to_all(send, "aa", 0, 0, tiled=True).reshape(-1, 3 * HD)
    dout = project_back(lax.all_gather(grad_out, "ba", axis=1, tiled=True), w_out).astype(jnp.bfloat16)
    dout = lax.all_to_all(by_head(dout), "aa", 0, 0, tiled=True).reshape(-1, HD)
    grads = one_head(qkv, dout, all_seg, scaling)
    back = lax.all_to_all(grads.reshape(heads, tok_count, 3 * HD), "aa", 0, 0, tiled=True)
    grad_q = back[:, :, 0:HD].transpose(1, 0, 2).reshape(tok_count, heads * HD)
    pairs = back[:, :, HD:].reshape(groups, 2, tok_count, 2 * HD).astype(jnp.float32).sum(axis=1)
    pairs = pairs.astype(jnp.bfloat16).transpose(1, 0, 2)
    grad_k = pairs[:, :, 0:HD].reshape(tok_count, groups * HD)
    grad_v = pairs[:, :, HD:].reshape(tok_count, groups * HD)
    partial_value = project_back(grad_q, w_query) + project_back(grad_k, w_key) + project_back(grad_v, w_value)
    return lax.psum_scatter(partial_value.astype(jnp.bfloat16), "ba", scatter_dimension=1, tiled=True)


def solution(mesh):
    return jax.shard_map(
        local,
        mesh=mesh,
        in_specs=(
            P("aa", "ba"),
            P("aa", "ba"),
            P("aa", "ba"),
            P("aa", "ba"),
            P("aa"),
            P(None, "ba"),
            P(None, "ba"),
            P(None, "ba"),
            P("ba", None),
        ),
        out_specs=P("aa", "ba"),
        check_vma=False,
    )
```

```python
import functools

import jax
import jax.numpy as jnp
from jax import lax
from jax.experimental import pallas as pl
from jax.experimental.pallas import tpu as pltpu
from jax.sharding import PartitionSpec as P

D = 5376
HQ = 32
HD = 128
DOCS = 6


NEG_FILL = -1e30


def from_behind(value, axis, steps):
    count = lax.axis_size(axis)
    pairs = [(source, (source + steps) % count) for source in range(count)]
    return lax.ppermute(value, axis, pairs)


def block_scores(query, dout, keys, values, query_pos, query_seg, key_pos, key_seg, scaling):
    row_count = query.shape[0]
    col_count = keys.shape[0]
    groups = keys.shape[1] // HD
    query_four = query.reshape(row_count, groups, 2, HD)
    dout_four = dout.reshape(row_count, groups, 2, HD)
    key_three = keys.reshape(col_count, groups, HD)
    value_three = values.reshape(col_count, groups, HD)
    scores = (
        jnp.einsum("iagd,jad->agij", query_four, key_three, preferred_element_type=jnp.float32)
        * scaling
    )
    dprobs = jnp.einsum(
        "iagd,jad->agij", dout_four, value_three, preferred_element_type=jnp.float32
    )
    allowed = (key_pos[None, :] <= query_pos[:, None]) & (key_seg[None, :] == query_seg[:, None])
    return (scores, dprobs, allowed, query_four, dout_four, key_three)


def forward_stats(
    query, dout, keys, values, query_pos, query_seg, key_pos, key_seg, scaling, state
):
    run_max, run_sum, run_dot = state
    scores, dprobs, allowed, unused_q, unused_d, unused_k = block_scores(
        query, dout, keys, values, query_pos, query_seg, key_pos, key_seg, scaling
    )
    masked = jnp.where(allowed, scores, NEG_FILL)
    new_max = jnp.maximum(run_max, jnp.max(masked, axis=-1))
    expo = jnp.where(allowed, jnp.exp(scores - new_max[..., None]), 0.0)
    return (new_max, jnp.sum(expo, axis=-1), jnp.sum(expo * dprobs, axis=-1))


def block_grads(
    query, dout, row_lse, row_delta, keys, values, query_pos, query_seg, key_pos, key_seg, scaling
):
    scores, dprobs, allowed, query_four, dout_four, key_three = block_scores(
        query, dout, keys, values, query_pos, query_seg, key_pos, key_seg, scaling
    )
    softmax_w = jnp.where(allowed, jnp.exp(scores - row_lse[..., None]), 0.0)
    dscores = softmax_w * (dprobs - row_delta[..., None])
    softmax_low = softmax_w.astype(jnp.bfloat16)
    dscores_low = dscores.astype(jnp.bfloat16)
    grad_v = jnp.einsum(
        "agij,iagd->jad", softmax_low, dout_four, preferred_element_type=jnp.float32
    )
    grad_k = (
        jnp.einsum("agij,iagd->jad", dscores_low, query_four, preferred_element_type=jnp.float32)
        * scaling
    )
    grad_q = (
        jnp.einsum("agij,jad->iagd", dscores_low, key_three, preferred_element_type=jnp.float32)
        * scaling
    )
    return (
        grad_q.reshape(query.shape[0], -1),
        grad_k.reshape(keys.shape[0], -1),
        grad_v.reshape(keys.shape[0], -1),
    )


def project_back(grad, weight):
    return lax.dot_general(
        grad, weight, (((1,), (1,)), ((), ())), preferred_element_type=jnp.float32
    )


def local_ring(query, keys, values, grad_out, segment_ids, w_query, w_key, w_value, w_out):
    seq_devices = lax.axis_size("aa")
    own_index = lax.axis_index("aa")
    tok_count = query.shape[0]
    scaling = (D / HQ) ** (-0.5)
    groups = keys.shape[1] // HD
    all_seg = lax.all_gather(segment_ids, "aa", axis=0, tiled=True)
    dout = project_back(lax.all_gather(grad_out, "ba", axis=1, tiled=True), w_out).astype(
        jnp.bfloat16
    )
    offsets = lax.iota(jnp.int32, tok_count)
    own_pos = own_index * tok_count + offsets
    own_seg = lax.dynamic_slice_in_dim(all_seg, own_index * tok_count, tok_count)
    stat_shape = (groups, 2, tok_count)
    stats_start = (
        jnp.full(stat_shape, NEG_FILL, jnp.float32),
        jnp.zeros(stat_shape, jnp.float32),
        jnp.zeros(stat_shape, jnp.float32),
    )
    piece = (
        lax.all_gather(keys, "aa", axis=0, tiled=True),
        lax.all_gather(values, "aa", axis=0, tiled=True),
    )
    width = piece[0].shape[0]
    key_pos = lax.iota(jnp.int32, width)
    key_seg = all_seg
    run_max, run_sum, run_dot = forward_stats(
        query, dout, piece[0], piece[1], own_pos, own_seg, key_pos, key_seg, scaling, stats_start
    )
    row_lse = run_max + jnp.log(run_sum)
    row_delta = run_dot / run_sum
    zero_q = jnp.zeros(query.shape, jnp.float32)
    zero_k = jnp.zeros(keys.shape, jnp.float32)

    def step_keys(step_index, state):
        (keys_now, values_now), (dk_now, dv_now), grad_q = state
        anchor = (own_index - step_index) % seq_devices
        key_pos = anchor * tok_count + offsets
        key_seg = lax.dynamic_slice_in_dim(all_seg, anchor * tok_count, tok_count)
        add_q, add_k, add_v = block_grads(
            query,
            dout,
            row_lse,
            row_delta,
            keys_now,
            values_now,
            own_pos,
            own_seg,
            key_pos,
            key_seg,
            scaling,
        )
        bundle_next = from_behind((keys_now, values_now), "aa", 1)
        sums_next = (
            from_behind((dk_now + add_k).astype(jnp.bfloat16), "aa", 1).astype(jnp.float32),
            from_behind((dv_now + add_v).astype(jnp.bfloat16), "aa", 1).astype(jnp.float32),
        )
        return (bundle_next, sums_next, grad_q + add_q)

    initial = ((keys, values), (zero_k, zero_k), zero_q)
    final = lax.fori_loop(0, seq_devices, step_keys, initial)
    grad_q = final[2]
    grad_k = final[1][0]
    grad_v = final[1][1]
    partial_value = (
        project_back(grad_q.astype(jnp.bfloat16), w_query)
        + project_back(grad_k.astype(jnp.bfloat16), w_key)
        + project_back(grad_v.astype(jnp.bfloat16), w_value)
    )
    return lax.psum_scatter(
        partial_value.astype(jnp.bfloat16), "ba", scatter_dimension=1, tiled=True
    )


def fold_rows(value, op):
    return op(value.reshape(-1, 8, value.shape[1]), axis=0)


CONTRACT_LAST = (((1,), (1,)), ((), ()))


def block_of(ref, kb, block, lanes):
    return ref[pl.ds(pl.multiple_of(kb * block, block), block), lanes]


def masked_scores(qkv_ref, query, qb, kb, block, starts, scaling):
    lane = lax.broadcasted_iota(jnp.int32, (block, block), 1)
    sub = lax.broadcasted_iota(jnp.int32, (block, block), 0)
    key = block_of(qkv_ref, kb, block, slice(HD, 2 * HD))
    s = lax.dot_general(key, query, CONTRACT_LAST, preferred_element_type=jnp.float32)
    key_pos = kb * block + sub
    allowed = (key_pos <= qb * block + lane) & (key_pos >= starts)
    return jnp.where(allowed, s * scaling, NEG_FILL)


def stats_kernel(block, scaling, low_ref, start_ref, qkv_ref, lse_ref, s_ref):
    def query_block(qb, carry):
        query = block_of(qkv_ref, qb, block, slice(0, HD))
        low = low_ref[qb]
        starts = start_ref[pl.ds(qb, 1), :]

        def scores_at(kb, top):
            s = masked_scores(qkv_ref, query, qb, kb, block, starts, scaling)
            s_ref[pl.ds(pl.multiple_of(kb * block, block), block), :] = s
            return jnp.maximum(top, fold_rows(s, jnp.max))

        top = lax.fori_loop(low, qb + 1, scores_at, jnp.full((8, block), NEG_FILL, jnp.float32))
        top = jnp.max(top, axis=0, keepdims=True)

        def sums_at(kb, run_sum):
            return run_sum + fold_rows(jnp.exp(block_of(s_ref, kb, block, slice(None)) - top), jnp.sum)

        run_sum = lax.fori_loop(low, qb + 1, sums_at, jnp.zeros((8, block), jnp.float32))
        lse_ref[pl.ds(qb, 1), :] = top + jnp.log(jnp.sum(run_sum, axis=0, keepdims=True))
        return carry

    lax.fori_loop(0, qkv_ref.shape[0] // block, query_block, 0)


def grads_kernel(block, scaling, low_ref, start_ref, lse_ref, qkv_ref, dout_ref, gq_ref, gkv_ref, p_ref, dp_ref, dk_ref, dv_ref):
    dk_ref[...] = jnp.zeros_like(dk_ref)
    dv_ref[...] = jnp.zeros_like(dv_ref)

    def query_block(qb, carry):
        rows = pl.ds(pl.multiple_of(qb * block, block), block)
        query = qkv_ref[rows, 0:HD]
        dout = dout_ref[rows, :]
        low = low_ref[qb]
        starts = start_ref[pl.ds(qb, 1), :]
        lse = lse_ref[pl.ds(qb, 1), :]

        def probs_at(kb, run_dot):
            cols = pl.ds(pl.multiple_of(kb * block, block), block)
            s = masked_scores(qkv_ref, query, qb, kb, block, starts, scaling)
            value = qkv_ref[cols, 2 * HD : 3 * HD]
            dp = lax.dot_general(value, dout, CONTRACT_LAST, preferred_element_type=jnp.float32)
            probs = jnp.exp(s - lse)
            p_ref[cols, :] = probs
            dp_ref[cols, :] = dp
            return run_dot + fold_rows(probs * dp, jnp.sum)

        run_dot = lax.fori_loop(low, qb + 1, probs_at, jnp.zeros((8, block), jnp.float32))
        delta = jnp.sum(run_dot, axis=0, keepdims=True)

        def grads_at(kb, grad_q):
            cols = pl.ds(pl.multiple_of(kb * block, block), block)
            probs = p_ref[cols, :]
            dscores = (probs * (dp_ref[cols, :] - delta)).astype(jnp.bfloat16)
            dv_ref[cols, :] += jnp.dot(probs.astype(jnp.bfloat16), dout, preferred_element_type=jnp.float32)
            dk_ref[cols, :] += jnp.dot(dscores, query, preferred_element_type=jnp.float32)
            return grad_q + lax.dot_general(
                dscores, qkv_ref[cols, HD : 2 * HD], (((0,), (0,)), ((), ())), preferred_element_type=jnp.float32
            )

        grad_q = lax.fori_loop(low, qb + 1, grads_at, jnp.zeros((block, HD), jnp.float32))
        gq_ref[rows, :] = (grad_q * scaling).astype(jnp.bfloat16)
        return carry

    lax.fori_loop(0, qkv_ref.shape[0] // block, query_block, 0)
    gkv_ref[:, 0:HD] = (dk_ref[...] * scaling).astype(jnp.bfloat16)
    gkv_ref[:, HD : 2 * HD] = dv_ref[...].astype(jnp.bfloat16)


def document_starts(all_seg, block):
    chosen = all_seg[None, :] == lax.iota(jnp.int32, DOCS)[:, None]
    firsts = jnp.sum(all_seg[None, :] < lax.iota(jnp.int32, DOCS)[:, None], axis=1, dtype=jnp.int32)
    starts = jnp.sum(jnp.where(chosen, firsts[:, None], 0), axis=0, dtype=jnp.int32).reshape(-1, block)
    return starts[:, 0] // block, starts


WHOLE = pl.BlockSpec(memory_space=pltpu.VMEM)
SCALARS = pl.BlockSpec(memory_space=pltpu.SMEM)


def head_stats(low, starts, qkv, scaling):
    total, block = qkv.shape[0], starts.shape[1]
    return pl.pallas_call(
        functools.partial(stats_kernel, block, scaling),
        out_shape=jax.ShapeDtypeStruct(starts.shape, jnp.float32),
        in_specs=[SCALARS, WHOLE, WHOLE],
        out_specs=WHOLE,
        scratch_shapes=[pltpu.VMEM((total, block), jnp.float32)],
        compiler_params=pltpu.CompilerParams(vmem_limit_bytes=16 * 1024 * 1024),
        cost_estimate=pl.CostEstimate(flops=total * total * HD, bytes_accessed=qkv.size * 2, transcendentals=total * total // 2),
        name="stats",
    )(low, starts, qkv)


def head_grads(low, starts, lse, qkv, dout, scaling):
    total, block = qkv.shape[0], starts.shape[1]
    return pl.pallas_call(
        functools.partial(grads_kernel, block, scaling),
        out_shape=[
            jax.ShapeDtypeStruct((total, HD), jnp.bfloat16),
            jax.ShapeDtypeStruct((total, 2 * HD), jnp.bfloat16),
        ],
        in_specs=[SCALARS, WHOLE, WHOLE, WHOLE, WHOLE],
        out_specs=[WHOLE, WHOLE],
        scratch_shapes=[
            pltpu.VMEM((total, block), jnp.float32),
            pltpu.VMEM((total, block), jnp.float32),
            pltpu.VMEM((total, HD), jnp.float32),
            pltpu.VMEM((total, HD), jnp.float32),
        ],
        compiler_params=pltpu.CompilerParams(vmem_limit_bytes=32 * 1024 * 1024),
        cost_estimate=pl.CostEstimate(flops=5 * total * total * HD, bytes_accessed=qkv.size * 6, transcendentals=total * total // 2),
        name="grads",
    )(low, starts, lse, qkv, dout)


def local(query, keys, values, grad_out, segment_ids, w_query, w_key, w_value, w_out):
    seq_devices = lax.axis_size("aa")
    tok_count = query.shape[0]
    heads = query.shape[1] // HD
    groups = keys.shape[1] // HD
    if heads != seq_devices:
        return local_ring(query, keys, values, grad_out, segment_ids, w_query, w_key, w_value, w_out)
    scaling = (D / HQ) ** (-0.5)
    block = 256 if (tok_count * seq_devices) % 256 == 0 else 128

    def by_head(value):
        return value.reshape(value.shape[0], -1, HD).transpose(1, 0, 2)

    def exchange(value):
        return lax.all_to_all(value, "aa", 0, 0, tiled=True)

    gathered = lax.all_gather(grad_out, "ba", axis=1, tiled=True)
    all_seg = lax.all_gather(segment_ids, "aa", axis=0, tiled=True)
    low, starts = document_starts(all_seg, block)
    send = jnp.concatenate(
        [by_head(query), jnp.repeat(by_head(keys), 2, axis=0), jnp.repeat(by_head(values), 2, axis=0)], axis=2
    )
    qkv = exchange(send).reshape(-1, 3 * HD)
    lse = head_stats(low, starts, qkv, scaling)
    gathered, lse = lax.optimization_barrier((gathered, lse))
    dout = exchange(by_head(project_back(gathered, w_out).astype(jnp.bfloat16))).reshape(-1, HD)
    grad_q, grad_kv = head_grads(low, starts, lse, qkv, dout, scaling)
    half = tok_count // 2
    odd = lax.axis_index("aa") % 2
    grad_kv = grad_kv.reshape(heads, 2, half, 2 * HD)
    own = lax.dynamic_index_in_dim(grad_kv, odd, 1, keepdims=False)
    other = lax.dynamic_index_in_dim(grad_kv, 1 - odd, 1, keepdims=False)
    other = lax.ppermute(other, "aa", [(source, source ^ 1) for source in range(seq_devices)])
    back_q = exchange(grad_q.reshape(heads, tok_count, HD))
    own = (own.astype(jnp.float32) + other.astype(jnp.float32)).astype(jnp.bfloat16)
    back_q, own = lax.optimization_barrier((back_q, own))
    back_kv = exchange(own).reshape(groups, 2 * half, 2 * HD).transpose(1, 0, 2)
    grad_q = back_q.transpose(1, 0, 2).reshape(tok_count, heads * HD)
    grad_k = back_kv[:, :, 0:HD].reshape(tok_count, groups * HD)
    grad_v = back_kv[:, :, HD:].reshape(tok_count, groups * HD)
    part = project_back(grad_q, w_query) + project_back(grad_k, w_key) + project_back(grad_v, w_value)
    return lax.psum_scatter(part.astype(jnp.bfloat16), "ba", scatter_dimension=1, tiled=True)


def solution(mesh):
    return jax.shard_map(
        local,
        mesh=mesh,
        in_specs=(
            P("aa", "ba"),
            P("aa", "ba"),
            P("aa", "ba"),
            P("aa", "ba"),
            P("aa"),
            P(None, "ba"),
            P(None, "ba"),
            P(None, "ba"),
            P("ba", None),
        ),
        out_specs=P("aa", "ba"),
        check_vma=False,
    )
```
